32 devices in a mesh: dp: 8 (over y, x, core), expert: 4 (over z).
Axes of the slice: x: 2, y: 2, z: 4, core: 2. Of those that a mesh axis runs over, the one named last changes fastest.
Arguments:
- policy_hidden: bfloat16 [1024, 4096], P('dp', 'expert'), may hold values from -6 to 6
- reference_hidden: bfloat16 [1024, 4096], P('dp', 'expert'), may hold values from -6 to 6
- policy_norm_gain: float32 [4096], P('expert'), may hold values from 0.25 to 1.75
- reference_norm_gain: float32 [4096], P('expert'), may hold values from 0.25 to 1.75
- policy_router: float32 [4096, 4], P('expert'), may hold values from -5.1875 to 5.1875
- reference_router: float32 [4096, 4], P('expert'), may hold values from -5.1875 to 5.1875
- policy_gate: bfloat16 [4, 4096, 8192], P('expert', 'dp'), may hold values from -0.09375 to 0.09375
- policy_up: bfloat16 [4, 4096, 8192], P('expert', 'dp'), may hold values from -0.09375 to 0.09375
- policy_down: bfloat16 [4, 8192, 4096], P('expert', 'dp'), may hold values from -0.0625 to 0.0625
- reference_gate: bfloat16 [4, 4096, 8192], P('expert', 'dp'), may hold values from -0.09375 to 0.09375
- reference_up: bfloat16 [4, 4096, 8192], P('expert', 'dp'), may hold values from -0.09375 to 0.09375
- reference_down: bfloat16 [4, 8192, 4096], P('expert', 'dp'), may hold values from -0.0625 to 0.0625
- expert_ids: int32 [1024, 2], P('dp'), may hold values from 0 to 3, all different within a row; in each aligned block of 128 rows (0 to 127, 128 to 255, ...) at most 96 rows name the same one
- lengths: int32 [32], P('dp'), may hold values from 1 to 32, as said below
Outputs:
- policy_mixture: bfloat16 [1024, 4096], P('dp', 'expert')
- reference_mixture: bfloat16 [1024, 4096], P('dp', 'expert')
- token_kl: float32 [1024], P('dp')
- loss: float32 [], replicated
The draws below stay inside these ranges and needn't reach their ends.
Inputs may be any that keep to these rules, and one draw needn't show every extreme that they name: `expert_ids`: each row names 2 different experts; among the rows of one index of dp (aligned blocks of 128 rows) no expert is named more than 96 times, and in some block one expert is named exactly 96 times. The first lengths[r] of rollout r's 32 positions are live.
All inputs are finite; a program needn't handle non-finite values.
Results may differ from the reference program's by a relative error of at most 0.02.
Values may be sent and summed in bfloat16 or wider, within the bound.
A program may use at most 256 MiB of HBM per device.

```python
import math
import jax
import jax.numpy as jnp
import numpy as np
from jax import lax

D = 4096
FF = 8192
TOP = 2
SEG = 32
TOK_DEV = 128
EXPERTS = 4
CAP = 96
TOKENS = 1024
N_DP = 8


def router_draw(key, stream_index):
    individual = jnp.clip(jax.random.normal(jax.random.fold_in(key, stream_index), (D, EXPERTS), jnp.float32), -4.0, 4.0) / math.sqrt(D)
    return individual


def draw_policy_router(key, part):
    return router_draw(key, 11)


def draw_reference_router(key, part):
    return router_draw(key, 12)


def draw_lengths(key, part):
    rollout_count = TOKENS // SEG
    per_block = TOK_DEV // SEG
    rollout_index = jnp.arange(rollout_count, dtype=jnp.int32)
    block_index = rollout_index // per_block
    block_total = rollout_count // per_block
    floor_limit = max(SEG // 3, 1)
    upper_limit = floor_limit + (SEG - floor_limit) * block_index // max(block_total - 1, 1)
    drawn = jax.random.randint(jax.random.fold_in(key, 5), (rollout_count,), 1, upper_limit + 1, dtype=jnp.int32)
    fullest = rollout_count - per_block
    drawn = jnp.where(rollout_index == fullest, jnp.int32(SEG), drawn)
    drawn = jnp.where(rollout_index == 0, jnp.int32(1), drawn)
    return drawn.astype(jnp.int32)


def levels(own_key, extent, pieces, low, high):
    level, own = 1.0, jax.random.fold_in(own_key, 6)
    for dim, parts in pieces:
        steps = jnp.exp(jax.random.uniform(jax.random.fold_in(own, dim), (parts,), jnp.float32, low / len(pieces), high / len(pieces)))
        level = level * jnp.repeat(steps, extent[dim] // parts).reshape([-1 if axis == dim else 1 for axis in range(len(extent))])
    return level


def deal_out(stream_key, own, number, rows, count, top, reach, lean):
    sequence = jax.random.permutation(stream_key, count)
    crowded, usual = load_shares(count, rows * top, reach, lean, True), load_shares(count, rows * top, reach, lean, False)
    places = jnp.arange(count)

    def named(sizes, turn):
        used = int((sizes > 0).sum())
        fixed = max(1, used // 4)
        passed = fixed + (places - fixed + turn * (used - fixed)) % max(1, count - fixed)
        return jnp.zeros((count,), jnp.int32).at[sequence[jnp.where(places < fixed, places, passed)]].set(jnp.asarray(sizes, jnp.int32))

    sizes = jnp.where(number % 4 == 0, named(crowded, number // 4), named(usual, number - number // 4 - 1))
    mixed = jax.random.permutation(jax.random.fold_in(own, 3), count)
    donor, sink = mixed[0:count // 2 * 2:2], mixed[1:count // 2 * 2:2]
    margin = jnp.minimum(sizes[donor] - 1, reach - sizes[sink]) // 2
    margin = jnp.where((donor == sequence[0]) | (sink == sequence[0]) | (sizes[sink] == 0), 0, jnp.maximum(margin, 0))
    passed = jax.random.randint(jax.random.fold_in(own, 4), (count // 2,), 0, 1 << 20) % (margin + 1)
    sizes = sizes.at[donor].add(-passed).at[sink].add(passed)
    labels = jnp.searchsorted(jnp.cumsum(sizes), jnp.arange(rows * top), side="right").astype(jnp.int32)
    listing = labels.reshape(top, rows).T
    listing = listing[jax.random.permutation(jax.random.fold_in(own, 1), rows)]
    turn = jax.random.randint(jax.random.fold_in(own, 2), (rows, 1), 0, top)
    return jnp.take_along_axis(listing, (jnp.arange(top)[None, :] + turn) % top, axis=1)


def load_shares(count, total, reach, lean, full):
    portions = [(1 << 20) // math.isqrt(rank ** lean) + 1 for rank in range(1, count + 1)]
    largest = reach if full else min(reach, max(-(-total // count), total * portions[0] // sum(portions)))
    least = 1 if total - largest >= count - 1 else 0
    holding, spare = [largest] + [least] * (count - 1), total - largest - least * (count - 1)
    while spare > 0:
        movable = [i for i in range(1, count) if holding[i] < largest] or [i for i in range(1, count) if holding[i] < reach]
        whole, left = sum([portions[i] for i in movable]), spare
        for i in movable:
            extra = min(reach - holding[i], max(1, left * portions[i] // whole), spare)
            holding[i] = holding[i] + extra
            spare = spare - extra
    return np.array(holding)


def scatter_about(own_key, dims, width, reach, split=(), kind=jnp.bfloat16):
    values = width * jax.random.normal(own_key, dims, jnp.float32)
    if split:
        values = values * levels(own_key, dims, split, -0.22, 0.18)
    return jnp.clip(values, -reach, reach).astype(kind)


def setup_inputs(seed: int = 0) -> dict:
    key_of = jax.random.split(jax.random.key(seed), 15)
    policy_hidden = scatter_about(key_of[0], (TOKENS, D), 1.0, 6.0, ((0, 8), (1, 4)))
    reference_hidden = scatter_about(key_of[1], (TOKENS, D), 1.0, 6.0, ((0, 8), (1, 4)))
    policy_norm_gain = jnp.clip(1.0 + 0.15 * jax.random.normal(key_of[2], (D,), jnp.float32), 0.25, 1.75)
    reference_norm_gain = jnp.clip(1.0 + 0.15 * jax.random.normal(key_of[3], (D,), jnp.float32), 0.25, 1.75)
    policy_router = draw_policy_router(jax.random.fold_in(key_of[14], 71), 0)
    reference_router = draw_reference_router(jax.random.fold_in(key_of[14], 71), 0)
    policy_gate = scatter_about(key_of[6], (EXPERTS, D, FF), D ** -0.5, 0.09375, ((0, 4), (1, 8)))
    policy_up = scatter_about(key_of[7], (EXPERTS, D, FF), D ** -0.5, 0.09375, ((0, 4), (1, 8)))
    policy_down = scatter_about(key_of[8], (EXPERTS, FF, D), FF ** -0.5, 0.0625, ((0, 4), (1, 8)))
    reference_gate = scatter_about(key_of[9], (EXPERTS, D, FF), D ** -0.5, 0.09375, ((0, 4), (1, 8)))
    reference_up = scatter_about(key_of[10], (EXPERTS, D, FF), D ** -0.5, 0.09375, ((0, 4), (1, 8)))
    reference_down = scatter_about(key_of[11], (EXPERTS, FF, D), FF ** -0.5, 0.0625, ((0, 4), (1, 8)))
    expert_ids_keys = jax.random.split(jax.random.fold_in(key_of[12], 1), TOKENS // TOK_DEV)
    expert_ids_turns = jax.random.permutation(jax.random.fold_in(key_of[12], 3), TOKENS // TOK_DEV)
    expert_ids = jax.vmap(lambda own, number: deal_out(jax.random.fold_in(key_of[12], 2), own, number, TOK_DEV, EXPERTS, TOP, CAP, 2))(expert_ids_keys, expert_ids_turns).reshape((TOKENS, TOP))
    lengths = draw_lengths(jax.random.fold_in(key_of[14], 71), 0)
    return {"policy_hidden": policy_hidden, "reference_hidden": reference_hidden, "policy_norm_gain": policy_norm_gain, "reference_norm_gain": reference_norm_gain, "policy_router": policy_router, "reference_router": reference_router, "policy_gate": policy_gate, "policy_up": policy_up, "policy_down": policy_down, "reference_gate": reference_gate, "reference_up": reference_up, "reference_down": reference_down, "expert_ids": expert_ids, "lengths": lengths}


EPSILON = 1e-05
KL_WEIGHT = 1.0
BALANCE_WEIGHT = 0.5

def normalize(hidden, norm_gain):
    values = hidden.astype(jnp.float32)
    meansq = lax.optimization_barrier(jnp.mean(values * values, axis=1, keepdims=True))
    return values * norm_gain * lax.rsqrt(meansq + EPSILON)

def expert_apply(operands):
    expert_rows, gate_weight, up_weight, down_weight = operands
    row_count = expert_rows.shape[0]
    gate_value = jnp.dot(expert_rows, gate_weight, preferred_element_type=jnp.float32)
    up_value = jnp.dot(expert_rows, up_weight, preferred_element_type=jnp.float32)
    hidden = (jax.nn.silu(gate_value) * up_value).astype(jnp.bfloat16)
    block_width = FF // N_DP
    hidden_blocks = hidden.reshape(row_count, N_DP, block_width).transpose(1, 0, 2)
    down_blocks = down_weight.reshape(N_DP, block_width, D)

    def add_block(running_total, operand_pair):
        block_part = jnp.dot(operand_pair[0], operand_pair[1], preferred_element_type=jnp.float32).astype(jnp.bfloat16)
        block_part = lax.optimization_barrier(block_part)
        return (running_total + block_part.astype(jnp.float32), None)
    running_total, _ = lax.scan(add_block, jnp.zeros((row_count, D), jnp.float32), (hidden_blocks, down_blocks))
    return running_total.astype(jnp.bfloat16)

def model_mixture(hidden, norm_gain, router, gate_weight, up_weight, down_weight, flat_slot, expert_ids, live_mask):
    normed = normalize(hidden, norm_gain)
    logits = jnp.dot(normed, router, precision=lax.Precision.HIGHEST)
    token_rows = normed.astype(jnp.bfloat16)
    route_rows = jnp.repeat(token_rows, TOP, axis=0)
    buffer = jnp.zeros((EXPERTS * N_DP * CAP, D), jnp.bfloat16).at[flat_slot].set(route_rows)
    buffer = buffer.reshape(EXPERTS, N_DP * CAP, D)
    outputs = lax.map(expert_apply, (buffer, gate_weight, up_weight, down_weight))
    picked = outputs.reshape(EXPERTS * N_DP * CAP, D)[flat_slot].reshape(TOKENS, TOP, D)
    matches = expert_ids[:, :, None] == jnp.arange(EXPERTS, dtype=jnp.int32)[None, None, :]
    chosen = lax.optimization_barrier(jnp.sum(jnp.where(matches, logits[:, None, :], 0.0), axis=2))
    gates = jax.nn.softmax(chosen, axis=1)
    mixed_rows = lax.optimization_barrier(jnp.sum(picked.astype(jnp.float32) * gates[:, :, None], axis=1)) * live_mask[:, None]
    return (mixed_rows.astype(jnp.bfloat16), logits)

def reference(policy_hidden, reference_hidden, policy_norm_gain, reference_norm_gain, policy_router, reference_router, policy_gate, policy_up, policy_down, reference_gate, reference_up, reference_down, expert_ids, lengths):
    position = jnp.arange(TOKENS, dtype=jnp.int32)
    live_mask = (position % SEG < jnp.repeat(lengths, SEG)).astype(jnp.float32)
    block_ids = expert_ids.reshape(N_DP, TOK_DEV * TOP)
    onehot = (block_ids[:, :, None] == jnp.arange(EXPERTS, dtype=jnp.int32)[None, None, :]).astype(jnp.int32)
    before = jnp.cumsum(onehot, axis=1) - onehot
    within = lax.optimization_barrier(jnp.sum(before * onehot, axis=2))
    block_index = jnp.arange(N_DP, dtype=jnp.int32)[:, None]
    flat_slot = (block_ids * (N_DP * CAP) + block_index * CAP + within).reshape(-1).astype(jnp.int32)
    policy_mixture, policy_logits = model_mixture(policy_hidden, policy_norm_gain, policy_router, policy_gate, policy_up, policy_down, flat_slot, expert_ids, live_mask)
    reference_mixture, reference_logits = model_mixture(reference_hidden, reference_norm_gain, reference_router, reference_gate, reference_up, reference_down, flat_slot, expert_ids, live_mask)
    policy_logprob = jax.nn.log_softmax(policy_logits, axis=1)
    reference_logprob = jax.nn.log_softmax(reference_logits, axis=1)
    policy_prob = jnp.exp(policy_logprob)
    token_kl = lax.optimization_barrier(jnp.sum(policy_prob * (policy_logprob - reference_logprob), axis=1)) * live_mask
    route_onehot = onehot.reshape(TOKENS, TOP, EXPERTS)
    counts = lax.optimization_barrier(jnp.sum(lax.optimization_barrier(jnp.sum(route_onehot, axis=1)).astype(jnp.float32) * live_mask[:, None], axis=0))
    probsum = lax.optimization_barrier(jnp.sum(policy_prob * live_mask[:, None], axis=0))
    kl_total = jnp.sum(token_kl)
    token_total = float(TOKENS)
    balance = EXPERTS * jnp.sum(counts / (TOP * token_total) * probsum / token_total)
    loss = KL_WEIGHT * kl_total / token_total + BALANCE_WEIGHT * balance
    return (policy_mixture, reference_mixture, token_kl, loss)
```

```python
import functools

import jax
import jax.numpy as jnp
from jax import lax
from jax.experimental import pallas as pl
from jax.experimental.pallas import tpu as pltpu
from jax.sharding import PartitionSpec as P

D = 4096
SEG = 32

EPSILON = 1e-05
KL_WEIGHT = 1.0
BALANCE_WEIGHT = 0.5

MESH = pl.DeviceIdType.MESH
VMEM = pl.BlockSpec(memory_space=pltpu.VMEM)
ANY = pl.BlockSpec(memory_space=pl.ANY)
VMEM_LIMIT = 67043328


def remote(src, dst, send_sem, recv_sem, dp, expert):
    return pltpu.make_async_remote_copy(
        src_ref=src,
        dst_ref=dst,
        send_sem=send_sem,
        recv_sem=recv_sem,
        device_id=(dp, expert),
        device_id_type=MESH,
    )


def greet(peers):
    barrier = pltpu.get_barrier_semaphore()
    for peer in peers:
        pl.semaphore_signal(barrier, inc=1, device_id=peer, device_id_type=MESH)
    pl.semaphore_wait(barrier, len(peers))


def around(index, size):
    return [lax.rem(index + step, size) for step in range(1, size)]


def small_kernel(n, z, terms_ref, counts_ref, all_terms, all_counts, sems):
    dp, ex = lax.axis_index("dp"), lax.axis_index("expert")
    ex_peers, dp_peers = around(ex, z), around(dp, n)
    greet([(dp, peer) for peer in ex_peers] + [(peer, ex) for peer in dp_peers])
    copies = []
    for step, peer in enumerate(dp_peers):
        copies.append(
            remote(counts_ref, all_counts.at[dp], sems.at[0, step], sems.at[1, step], peer, ex)
        )
    for step, peer in enumerate(ex_peers):
        at = n - 1 + step
        copies.append(
            remote(terms_ref, all_terms.at[ex], sems.at[0, at], sems.at[1, at], dp, peer)
        )
    for copy in copies:
        copy.start()
    all_counts[dp] = counts_ref[...]
    all_terms[ex] = terms_ref[...]
    for copy in copies:
        copy.wait()


def small_exchange(n, z, terms, counts):
    return pl.pallas_call(
        functools.partial(small_kernel, n, z),
        out_shape=(
            jax.ShapeDtypeStruct((z,) + terms.shape, terms.dtype),
            jax.ShapeDtypeStruct((n,) + counts.shape, counts.dtype),
        ),
        in_specs=[VMEM] * 2,
        out_specs=(VMEM,) * 2,
        scratch_shapes=[pltpu.SemaphoreType.DMA((2, n + z - 2))],
        compiler_params=pltpu.CompilerParams(collective_id=0, has_side_effects=True),
        name="small_exchange",
    )(terms, counts)


def entry_kernel(n, z, placed, out, relay, send_one, recv_one, send_two, recv_two):
    dp, ex = lax.axis_index("dp"), lax.axis_index("expert")
    halves = n // z
    cap, width = relay.shape[2], relay.shape[3]
    ex_peers, dp_peers = around(ex, z), around(dp, n)
    greet([(dp, peer) for peer in ex_peers] + [(peer, ex) for peer in dp_peers])

    def slots(expert, model, half):
        rows = pl.ds(pl.multiple_of(expert * cap, cap), cap)
        return placed.at[rows, pl.ds((model * halves + half) * width, width)]

    def landing(model, block):
        return out.at[model, pl.ds(pl.multiple_of(block * cap, cap), cap), :]

    first = []
    for model in range(2):
        for step, peer in enumerate(ex_peers):
            for half in range(halves):
                copy = remote(
                    slots(peer, model, half),
                    relay.at[model, ex * halves + half],
                    send_one.at[model, step, half],
                    recv_one.at[model, ex * halves + half],
                    dp,
                    peer,
                )
                copy.start()
                first.append(copy)

    def second(model, block, source):
        return remote(
            source,
            landing(model, dp),
            send_two.at[model, block],
            recv_two.at[model, dp],
            block,
            ex,
        )

    def forward(model, block, source):
        @pl.when(block != dp)
        def _():
            second(model, block, source).start()

        @pl.when(block == dp)
        def _():
            landing(model, dp)[...] = source[...]

    for model in range(2):
        for half in range(halves):
            forward(model, ex * halves + half, slots(ex, model, half))
        for step, peer in enumerate(reversed(ex_peers)):
            for half in range(halves):
                block = peer * halves + half
                remote(
                    relay.at[model, block],
                    relay.at[model, block],
                    send_one.at[model, 0, half],
                    recv_one.at[model, block],
                    dp,
                    peer,
                ).wait_recv()
                forward(model, block, relay.at[model, block])
    for model in range(2):
        for peer in dp_peers:
            remote(
                landing(model, peer),
                landing(model, peer),
                send_two.at[model, peer],
                recv_two.at[model, peer],
                peer,
                ex,
            ).wait_recv()
            second(model, peer, relay.at[model, peer]).wait_send()
    for copy in first:
        copy.wait_send()


def entry_exchange(n, z, cap, width, placed):
    halves = n // z
    return pl.pallas_call(
        functools.partial(entry_kernel, n, z),
        out_shape=jax.ShapeDtypeStruct((2, n * cap, width), placed.dtype),
        in_specs=[VMEM],
        out_specs=VMEM,
        scratch_shapes=[
            pltpu.VMEM((2, n, cap, width), placed.dtype),
            pltpu.SemaphoreType.DMA((2, z - 1, halves)),
            pltpu.SemaphoreType.DMA((2, n)),
            pltpu.SemaphoreType.DMA((2, n)),
            pltpu.SemaphoreType.DMA((2, n)),
        ],
        compiler_params=pltpu.CompilerParams(collective_id=1, has_side_effects=True),
        name="entry_exchange",
    )(placed)


def exit_kernel(
    n, z, rows_ref, stats_ref, out, all_stats, relay, send_one, recv_one, send_two, recv_two, sems
):
    dp, ex = lax.axis_index("dp"), lax.axis_index("expert")
    halves = n // z
    cap, width = relay.shape[2], relay.shape[3]
    ex_peers, dp_peers = around(ex, z), around(dp, n)
    greet([(dp, peer) for peer in ex_peers] + [(peer, ex) for peer in dp_peers])

    def source(model, block):
        return rows_ref.at[model, pl.ds(pl.multiple_of(block * cap, cap), cap), :]

    def landing(model, expert, half):
        rows = pl.ds(pl.multiple_of(expert * cap, cap), cap)
        return out.at[model, rows, pl.ds(pl.multiple_of(half * width, width), width)]

    stats = []
    for step, peer in enumerate(dp_peers):
        copy = remote(stats_ref, all_stats.at[dp], sems.at[0, step], sems.at[1, step], peer, ex)
        copy.start()
        stats.append(copy)
    first = []
    for model in range(2):
        for step, peer in enumerate(dp_peers):
            copy = remote(
                source(model, peer),
                relay.at[model, dp],
                send_one.at[model, step],
                recv_one.at[model, dp],
                peer,
                ex,
            )
            copy.start()
            first.append(copy)
    all_stats[dp] = stats_ref[...]

    def second(model, block, origin):
        return remote(
            origin,
            landing(model, ex, lax.rem(block, halves)),
            send_two.at[model, block],
            recv_two.at[model, ex, lax.rem(block, halves)],
            dp,
            block // halves,
        )

    def forward(model, block, origin):
        @pl.when(block // halves != ex)
        def _():
            second(model, block, origin).start()

        @pl.when(block // halves == ex)
        def _():
            landing(model, ex, lax.rem(block, halves))[...] = origin[...]

    for model in range(2):
        forward(model, dp, source(model, dp))
        for peer in reversed(dp_peers):
            remote(
                relay.at[model, peer],
                relay.at[model, peer],
                send_one.at[model, 0],
                recv_one.at[model, peer],
                peer,
                ex,
            ).wait_recv()
            forward(model, peer, relay.at[model, peer])
    for model in range(2):
        for peer in ex_peers:
            for half in range(halves):
                remote(
                    landing(model, peer, half),
                    landing(model, peer, half),
                    send_two.at[model, peer * halves + half],
                    recv_two.at[model, peer, half],
                    dp,
                    peer,
                ).wait_recv()
                second(
                    model, peer * halves + half, relay.at[model, peer * halves + half]
                ).wait_send()
    for copy in first:
        copy.wait_send()
    for copy in stats:
        copy.wait()


def exit_exchange(n, z, cap, width, rows, stats):
    halves = n // z
    return pl.pallas_call(
        functools.partial(exit_kernel, n, z),
        out_shape=(
            jax.ShapeDtypeStruct((2, z * cap, halves * width), rows.dtype),
            jax.ShapeDtypeStruct((n,) + stats.shape, stats.dtype),
        ),
        in_specs=[VMEM] * 2,
        out_specs=(VMEM,) * 2,
        scratch_shapes=[
            pltpu.VMEM((2, n, cap, width), rows.dtype),
            pltpu.SemaphoreType.DMA((2, n - 1)),
            pltpu.SemaphoreType.DMA((2, n)),
            pltpu.SemaphoreType.DMA((2, n)),
            pltpu.SemaphoreType.DMA((2, z, halves)),
            pltpu.SemaphoreType.DMA((2, n - 1)),
        ],
        compiler_params=pltpu.CompilerParams(collective_id=2, has_side_effects=True),
        name="exit_exchange",
    )(rows, stats)


class Plan:
    def __init__(self, n, blocks_up, blocks_down):
        self.levels = n.bit_length() - 1
        self.lags = [0] + [2 * p - 1 for p in range(1, self.levels + 1)]
        last = self.lags[-1]
        self.gu = 2 * blocks_up
        self.dn = blocks_down
        self.down0 = self.gu - 1 + last
        self.rest = self.down0 + self.dn
        self.end = 2 * self.gu + self.dn
        self.down1 = self.end - 1 + last
        self.ids = self.down1 + self.dn
        self.units = self.end + self.dn
        self.steps = self.ids + last

    def is_gu(self, u):
        return ((u >= 0) & (u < self.down0)) | ((u >= self.rest) & (u < self.end))

    def is_dn(self, u):
        return ((u >= self.down0) & (u < self.rest)) | ((u >= self.down1) & (u < self.ids))

    def gu_at(self, u):
        index = jnp.where(u < self.down0, u, u - self.dn)
        inner = lax.rem(index, self.gu)
        return index // self.gu, inner // 2, lax.rem(inner, 2)

    def dn_at(self, u):
        late = u >= self.rest
        return jnp.where(late, 1, 0), jnp.where(late, u - self.down1, u - self.down0)

    def buffer(self, u):
        return jnp.where(u < self.end, u, u - (self.down1 - self.end))


def expert_kernel(n, plan, rows_ref, gate0, up0, down0, gate1, up1, down1, out_ref, *scratch):
    levels, lags = plan.levels, plan.lags
    sends, recvs, keeps = scratch[:levels], scratch[levels : 2 * levels], scratch[2 * levels : 3 * levels - 1]
    wide, tall, hidden, gated, wsem, ssem, rsem = scratch[3 * levels - 1 :]
    me, ex = lax.axis_index("dp"), lax.axis_index("expert")
    w = wide.shape[-1]
    depth, width = gate0.shape[0], down0.shape[0]
    send_slots, keep_slots = sends[0].shape[0], keeps[0].shape[0]

    def bit(stride):
        return lax.rem(me // stride, 2)

    def partner(stride):
        return me + stride * (1 - 2 * bit(stride))

    def tiles(half, u, ref, block, span, held):
        low = bit(1)
        parity = 1 - low if half == 0 else low
        slot = lax.rem(u, 2)
        for q in range(n // 2):
            start = pl.multiple_of((2 * q + parity) * span + block * w, w)
            yield pltpu.make_async_copy(
                ref.at[:, pl.ds(start, w)], held.at[half, slot, q], wsem.at[half, slot, q]
            )

    def fetch(half, u):
        model, block, which = plan.gu_at(u)
        for m, g, ref in ((0, 0, gate0), (0, 1, up0), (1, 0, gate1), (1, 1, up1)):

            @pl.when(plan.is_gu(u) & (model == m) & (which == g))
            def _():
                for copy in tiles(half, u, ref, block, width, wide):
                    copy.start()

        dn_model, dn_block = plan.dn_at(u)
        for m, ref in ((0, down0), (1, down1)):

            @pl.when(plan.is_dn(u) & (dn_model == m))
            def _():
                for copy in tiles(half, u, ref, dn_block, depth, tall):
                    copy.start()

    def arrived(half, u):
        for condition, ref, span, held in (
            (plan.is_gu(u), gate0, width, wide),
            (plan.is_dn(u), down0, depth, tall),
        ):

            @pl.when(condition)
            def _():
                for copy in tiles(half, u, ref, 0, span, held):
                    copy.wait()

    def gu_product(u, half, q):
        model, _, _ = plan.gu_at(u)
        return jnp.dot(
            rows_ref[model],
            wide[half, lax.rem(u, 2), q],
            preferred_element_type=jnp.float32,
        )

    def dn_product(u, half, q):
        model, _ = plan.dn_at(u)
        return jnp.dot(
            hidden[model],
            tall[half, lax.rem(u, 2), q],
            preferred_element_type=jnp.float32,
        )

    def placing(p, u):
        color = lax.rem(u, 2)
        one, two = bit(2**p), bit(2 ** (levels - p))
        mine = one + color * (two - one)
        top = 2 ** (levels - p - 1)

        def place(r, keep):
            value = mine if keep else 1 - mine
            return r * (2 - color) + value * (1 + color * (top - 1))

        return place

    def hop(p, u):
        color = lax.rem(u, 2)
        one, two = partner(2 ** p), partner(2 ** (levels - p) if p else 1)
        return remote(
            sends[p].at[lax.rem(u, send_slots)],
            recvs[p].at[plan.buffer(u)],
            ssem.at[p, lax.rem(u, send_slots)],
            rsem.at[p, plan.buffer(u)],
            one + color * (two - one),
            ex,
        )

    def level_zero(u):
        arrived(0, u)
        slot = lax.rem(u, send_slots)
        for condition, product in ((plan.is_gu(u), gu_product), (plan.is_dn(u), dn_product)):

            @pl.when(condition)
            def _():
                for q in range(n // 2):
                    sends[0][slot, q] = product(u, 0, q).astype(jnp.bfloat16)
                hop(0, u).start()

    def level_one(u):
        arrived(1, u)
        slot, kept, buffer = lax.rem(u, send_slots), lax.rem(u, keep_slots), plan.buffer(u)
        place = placing(1, u)
        for condition, product in ((plan.is_gu(u), gu_product), (plan.is_dn(u), dn_product)):

            @pl.when(condition)
            def _():
                hop(0, u).wait_recv()
                for keep in (False, True):
                    for r in range(n // 4):
                        at = place(r, keep)
                        total = product(u, 1, at) + recvs[0][buffer, at].astype(jnp.float32)
                        if keep:
                            keeps[0][kept, r] = total.astype(jnp.bfloat16)
                        else:
                            sends[1][slot, r] = total.astype(jnp.bfloat16)
                    if not keep:
                        hop(1, u).start()

    def level(p, u):
        slot, kept, buffer = lax.rem(u, send_slots), lax.rem(u, keep_slots), plan.buffer(u)
        place = placing(p, u)

        @pl.when(plan.is_gu(u) | plan.is_dn(u))
        def _():
            hop(p - 1, u).wait_recv()
            for keep in (False, True):
                for r in range(n // 2 ** (p + 1)):
                    at = place(r, keep)
                    total = keeps[p - 2][kept, at].astype(jnp.float32) + recvs[p - 1][
                        buffer, at
                    ].astype(jnp.float32)
                    if keep:
                        keeps[p - 1][kept, r] = total.astype(jnp.bfloat16)
                    else:
                        sends[p][slot, r] = total.astype(jnp.bfloat16)
                if not keep:
                    hop(p, u).start()

    def finish(u):
        kept, buffer = lax.rem(u, keep_slots), plan.buffer(u)

        def total():
            return keeps[-1][kept, 0].astype(jnp.float32) + recvs[-1][buffer, 0].astype(jnp.float32)

        @pl.when(plan.is_gu(u) | plan.is_dn(u))
        def _():
            hop(levels - 1, u).wait_recv()

        model, block, which = plan.gu_at(u)

        @pl.when(plan.is_gu(u) & (which == 0))
        def _():
            gated[...] = total()

        @pl.when(plan.is_gu(u) & (which == 1))
        def _():
            value = gated[...]
            hidden[model, :, pl.ds(pl.multiple_of(block * w, w), w)] = (
                value / (1.0 + jnp.exp(-value)) * total()
            ).astype(jnp.bfloat16)

        dn_model, dn_block = plan.dn_at(u)

        @pl.when(plan.is_dn(u))
        def _():
            out_ref[dn_model, :, pl.ds(pl.multiple_of(dn_block * w, w), w)] = total().astype(
                jnp.bfloat16
            )

        @pl.when(plan.is_gu(u) | plan.is_dn(u))
        def _():
            for p in range(levels):
                hop(p, u).wait_send()

    fetch(0, jnp.int32(0))
    greet([(partner(2**p), ex) for p in range(levels)])

    def step(t, carry):
        fetch(0, t + 1)
        fetch(1, t)
        finish(t - lags[levels])
        for p in range(levels - 1, 1, -1):
            level(p, t - lags[p])
        level_one(t - lags[1])
        level_zero(t)
        return carry

    lax.fori_loop(0, plan.steps, step, 0)


def experts(n, rows, weights):
    (gate0, up0, down0), (gate1, up1, down1) = weights
    _, chunk, depth = rows.shape
    width = down0.shape[0]
    w = depth // 2
    plan = Plan(n, width // w, depth // w)
    levels = plan.levels
    if 2**levels != n or levels < 2:
        raise ValueError("dp size")
    send_slots, keep_slots = plan.lags[-1] + 1, 4
    bf = jnp.bfloat16
    parts = [n // 2 ** (p + 1) for p in range(levels)]
    flops = 2 * chunk * 3 * depth * n * width * 2
    return pl.pallas_call(
        functools.partial(expert_kernel, n, plan),
        out_shape=jax.ShapeDtypeStruct((2, chunk, depth), bf),
        in_specs=[VMEM] + [ANY] * 6,
        out_specs=VMEM,
        scratch_shapes=[pltpu.VMEM((send_slots, part, chunk, w), bf) for part in parts]
        + [pltpu.VMEM((plan.units, part, chunk, w), bf) for part in parts]
        + [pltpu.VMEM((keep_slots, part, chunk, w), bf) for part in parts[1:]]
        + [
            pltpu.VMEM((2, 2, n // 2, depth, w), bf),
            pltpu.VMEM((2, 2, n // 2, width, w), bf),
            pltpu.VMEM((2, chunk, width), bf),
            pltpu.VMEM((chunk, w), jnp.float32),
            pltpu.SemaphoreType.DMA((2, 2, n // 2)),
            pltpu.SemaphoreType.DMA((levels, send_slots)),
            pltpu.SemaphoreType.DMA((levels, plan.units)),
        ],
        compiler_params=pltpu.CompilerParams(
            collective_id=3, has_side_effects=True, vmem_limit_bytes=VMEM_LIMIT
        ),
        cost_estimate=pl.CostEstimate(flops=flops, bytes_accessed=12 * depth * n * width, transcendentals=0),
        name="experts",
    )(rows, gate0, up0, down0, gate1, up1, down1)


def per_device(
    policy_hidden,
    reference_hidden,
    policy_norm_gain,
    reference_norm_gain,
    policy_router,
    reference_router,
    policy_gate,
    policy_up,
    policy_down,
    reference_gate,
    reference_up,
    reference_down,
    expert_ids,
    lengths,
):
    n, z = lax.axis_size("dp"), lax.axis_size("expert")
    ex = lax.axis_index("expert")
    tokens, features = policy_hidden.shape
    routes = expert_ids.shape[1]
    cap = 3 * tokens // z
    depth = policy_gate.shape[1]
    token_total = float(tokens * n)
    f32, bf = jnp.float32, jnp.bfloat16

    live = (jnp.arange(SEG, dtype=jnp.int32)[None, :] < lengths[:, None]).reshape(-1)
    live_f = live.astype(f32)
    flat_ids = expert_ids.reshape(-1)
    flat_live = jnp.repeat(live, routes)
    choice = flat_ids[:, None] == jnp.arange(z, dtype=jnp.int32)[None, :]
    onehot = (choice & flat_live[:, None]).astype(bf)
    order = jnp.arange(tokens * routes, dtype=jnp.int32)
    earlier = (order[None, :] < order[:, None]).astype(bf)
    before = jnp.dot(earlier, onehot, preferred_element_type=f32)
    pos = jnp.sum(before * choice.astype(f32), axis=1).astype(jnp.int32)
    target = jnp.where(flat_live, flat_ids * cap + pos, -1).reshape(tokens, routes)
    counts = jnp.sum(onehot.astype(f32), axis=0)
    counts_tile = jnp.pad(counts[None, :], ((0, 7), (0, 128 - z)))

    def router_terms(hidden, gain, router):
        values = hidden.astype(f32)
        logits = lax.dot_general(
            router, values * gain, (((0,), (1,)), ((), ())), precision=lax.Precision.HIGHEST
        )
        return jnp.concatenate((logits, jnp.sum(values * values, axis=1)[None, :]), axis=0)

    terms = jnp.concatenate(
        (
            router_terms(policy_hidden, policy_norm_gain, policy_router),
            router_terms(reference_hidden, reference_norm_gain, reference_router),
        ),
        axis=0,
    )
    terms = jnp.pad(terms, ((0, -terms.shape[0] % 8), (0, 0)))
    all_terms, all_counts = small_exchange(n, z, terms, counts_tile)
    terms = jnp.sum(all_terms, axis=0)
    block_counts = all_counts[:, 0, :z].astype(jnp.int32)

    def model_terms(base, hidden, gain):
        scale = lax.rsqrt(terms[base + z] / (n * depth) + EPSILON)
        logits = terms[base : base + z] * scale[None, :]
        rows = (hidden.astype(f32) * gain * scale[:, None]).astype(bf)
        return logits, rows

    policy_logits, policy_rows = model_terms(0, policy_hidden, policy_norm_gain)
    reference_logits, reference_rows = model_terms(z + 1, reference_hidden, reference_norm_gain)

    slot = jnp.arange(z * cap, dtype=jnp.int32)
    picks = [(target[:, k][:, None] == slot[None, :]).astype(bf) for k in range(routes)]
    select = sum(slot[:, None] == target[:, k][None, :] for k in range(routes)).astype(bf)
    stacked = jnp.concatenate((policy_rows, reference_rows), axis=1)
    placed = jnp.dot(select, stacked, preferred_element_type=f32).astype(bf)
    slot_rows = entry_exchange(n, z, cap, depth, placed)

    totals = jnp.sum(block_counts, axis=0)
    mine = lax.dynamic_slice_in_dim(block_counts, ex, 1, axis=1)[:, 0]
    first = jnp.cumsum(mine) - mine
    within = jnp.arange(cap, dtype=jnp.int32)
    packed = jnp.where(
        within[None, :] < mine[:, None], first[:, None] + within[None, :], -1
    ).reshape(-1)
    chunk = -(-5 * n * cap // 12 // 16) * 16
    weights = (
        (policy_gate[0], policy_up[0], policy_down[0]),
        (reference_gate[0], reference_up[0], reference_down[0]),
    )

    def body(index, results):
        wanted = index * chunk + jnp.arange(chunk, dtype=jnp.int32)
        gather = (wanted[:, None] == packed[None, :]).astype(bf)
        rows = lax.dot_general(
            slot_rows, gather, (((1,), (1,)), ((), ())), preferred_element_type=f32
        )
        rows = rows.astype(bf).transpose(0, 2, 1)
        outs = experts(n, rows, weights)
        spread = (packed[:, None] == wanted[None, :]).astype(bf)
        return results + jnp.einsum(
            "sr,mrd->msd", spread, outs, preferred_element_type=f32
        ).astype(bf)

    passes = (jnp.max(totals) + chunk - 1) // chunk
    results = lax.fori_loop(0, passes, body, jnp.zeros((2, n * cap, depth), bf))

    policy_logprob = jax.nn.log_softmax(policy_logits, axis=0)
    reference_logprob = jax.nn.log_softmax(reference_logits, axis=0)
    policy_prob = jnp.exp(policy_logprob)
    token_kl = jnp.sum(policy_prob * (policy_logprob - reference_logprob), axis=0) * live_f
    probsum = jnp.sum(policy_prob * live_f[None, :], axis=1)
    stats = jnp.concatenate((probsum, jnp.sum(token_kl)[None]))
    stats_tile = jnp.pad(stats[None, :], ((0, 7), (0, 128 - z - 1)))

    arrived, all_stats = exit_exchange(n, z, cap, depth, results, stats_tile)

    def combine(model, logits):
        matches = expert_ids[:, :, None] == jnp.arange(z, dtype=jnp.int32)[None, None, :]
        chosen = jnp.sum(jnp.where(matches, logits.T[:, None, :], 0.0), axis=2)
        gates = jax.nn.softmax(chosen, axis=1)
        total = 0.0
        for k in range(routes):
            picked = jnp.dot(picks[k], arrived[model], preferred_element_type=f32)
            total = total + picked * gates[:, k : k + 1]
        return (total * live_f[:, None]).astype(bf)

    policy_mixture = combine(0, policy_logits)
    reference_mixture = combine(1, reference_logits)
    stats = jnp.sum(all_stats[:, 0, :], axis=0)
    balance = z * jnp.sum(
        totals.astype(f32) / (routes * token_total) * stats[:z] / token_total
    )
    loss = KL_WEIGHT * stats[z] / token_total + BALANCE_WEIGHT * balance
    return (policy_mixture, reference_mixture, token_kl, loss)


def solution(mesh):
    in_specs = (
        P("dp", "expert"),
        P("dp", "expert"),
        P("expert"),
        P("expert"),
        P("expert", None),
        P("expert", None),
        P("expert", "dp", None),
        P("expert", "dp", None),
        P("expert", "dp", None),
        P("expert", "dp", None),
        P("expert", "dp", None),
        P("expert", "dp", None),
        P("dp", None),
        P("dp"),
    )
    out_specs = (P("dp", "expert"), P("dp", "expert"), P("dp"), P())
    return jax.shard_map(
        per_device, mesh=mesh, in_specs=in_specs, out_specs=out_specs, check_vma=False
    )
```

```python
import functools

import jax
import jax.numpy as jnp
from jax import lax
from jax.experimental import pallas as pl
from jax.experimental.pallas import tpu as pltpu
from jax.sharding import PartitionSpec as P

D = 4096
SEG = 32

EPSILON = 1e-05
KL_WEIGHT = 1.0
BALANCE_WEIGHT = 0.5
SIZES = ((4, 18), (5, 19), (6, 20))

MESH = pl.DeviceIdType.MESH
VMEM = pl.BlockSpec(memory_space=pltpu.VMEM)
ANY = pl.BlockSpec(memory_space=pl.ANY)
VMEM_LIMIT = 67043328


def remote(src, dst, send_sem, recv_sem, dp, expert):
    return pltpu.make_async_remote_copy(
        src_ref=src,
        dst_ref=dst,
        send_sem=send_sem,
        recv_sem=recv_sem,
        device_id=(dp, expert),
        device_id_type=MESH,
    )


def greet(peers):
    barrier = pltpu.get_barrier_semaphore()
    for peer in peers:
        pl.semaphore_signal(barrier, inc=1, device_id=peer, device_id_type=MESH)
    pl.semaphore_wait(barrier, len(peers))


def around(index, size):
    return [lax.rem(index + step, size) for step in range(1, size)]


def small_kernel(n, z, terms_ref, counts_ref, all_terms, all_counts, sems):
    dp, ex = lax.axis_index("dp"), lax.axis_index("expert")
    ex_peers, dp_peers = around(ex, z), around(dp, n)
    greet([(dp, peer) for peer in ex_peers] + [(peer, ex) for peer in dp_peers])
    copies = []
    for step, peer in enumerate(dp_peers):
        copies.append(
            remote(counts_ref, all_counts.at[dp], sems.at[0, step], sems.at[1, step], peer, ex)
        )
    for step, peer in enumerate(ex_peers):
        at = n - 1 + step
        copies.append(
            remote(terms_ref, all_terms.at[ex], sems.at[0, at], sems.at[1, at], dp, peer)
        )
    for copy in copies:
        copy.start()
    all_counts[dp] = counts_ref[...]
    all_terms[ex] = terms_ref[...]
    for copy in copies:
        copy.wait()


def small_exchange(n, z, terms, counts):
    return pl.pallas_call(
        functools.partial(small_kernel, n, z),
        out_shape=(
            jax.ShapeDtypeStruct((z,) + terms.shape, terms.dtype),
            jax.ShapeDtypeStruct((n,) + counts.shape, counts.dtype),
        ),
        in_specs=[VMEM] * 2,
        out_specs=(VMEM,) * 2,
        scratch_shapes=[pltpu.SemaphoreType.DMA((2, n + z - 2))],
        compiler_params=pltpu.CompilerParams(collective_id=0, has_side_effects=True),
        name="small_exchange",
    )(terms, counts)


class Plan:
    def __init__(self, n, blocks_up, blocks_down):
        self.levels = n.bit_length() - 1
        self.lags = [0] + [2 * p - 1 for p in range(1, self.levels + 1)]
        last = self.lags[-1]
        self.gu = 2 * blocks_up
        self.dn = blocks_down
        self.down0 = self.gu - 1 + last
        self.rest = self.down0 + self.dn
        self.end = 2 * self.gu + self.dn
        self.down1 = self.end - 1 + last
        self.ids = self.down1 + self.dn
        self.units = self.end + self.dn
        self.steps = self.ids + last
        self.leave0 = max(self.rest - 1 + last, self.end - 1 + self.lags[-2])
        self.each = -(-n // (self.steps - self.leave0 - 1))

    def is_gu(self, u):
        return ((u >= 0) & (u < self.down0)) | ((u >= self.rest) & (u < self.end))

    def is_dn(self, u):
        return ((u >= self.down0) & (u < self.rest)) | ((u >= self.down1) & (u < self.ids))

    def gu_at(self, u):
        index = jnp.where(u < self.down0, u, u - self.dn)
        inner = lax.rem(index, self.gu)
        return index // self.gu, inner // 2, lax.rem(inner, 2)

    def dn_at(self, u):
        late = u >= self.rest
        return jnp.where(late, 1, 0), jnp.where(late, u - self.down1, u - self.down0)

    def buffer(self, u):
        return jnp.where(u < self.end, u, u - (self.down1 - self.end))


def expert_kernel(
    n,
    z,
    plan,
    placed,
    gather_ref,
    spread_ref,
    stats_ref,
    gate0,
    up0,
    down0,
    gate1,
    up1,
    down1,
    arrived_ref,
    all_stats,
    *scratch,
):
    levels, lags = plan.levels, plan.lags
    sends, recvs = scratch[:levels], scratch[levels : 2 * levels]
    keeps = scratch[2 * levels : 3 * levels - 1]
    (
        wide,
        tall,
        hidden,
        gated,
        wsem,
        ssem,
        rsem,
        entry_relay,
        entry_slots,
        rows_ref,
        outs,
        exit_slots,
        exit_relay,
        stats_sem,
        in_send,
        in_recv,
        in_send2,
        in_recv2,
        out_send,
        out_recv,
        out_send2,
        out_recv2,
    ) = scratch[3 * levels - 1 :]
    me, ex = lax.axis_index("dp"), lax.axis_index("expert")
    w = wide.shape[-1]
    depth, width = gate0.shape[0], down0.shape[0]
    send_slots, keep_slots = sends[0].shape[0], keeps[0].shape[0]
    halves, cap = n // z, entry_relay.shape[2]
    ex_peers, dp_peers = around(ex, z), around(me, n)

    def block_rows(ref, model, block):
        return ref.at[model, pl.ds(pl.multiple_of(block * cap, cap), cap), :]


    def placed_at(expert, model, half):
        rows = pl.ds(pl.multiple_of(expert * cap, cap), cap)
        return placed.at[rows, pl.ds((model * halves + half) * depth, depth)]

    def entry_first(model, step, half):
        return remote(
            placed_at(ex_peers[step], model, half),
            entry_relay.at[model, ex * halves + half],
            in_send.at[model, step, half],
            in_recv.at[model, ex * halves + half],
            me,
            ex_peers[step],
        )

    def entry_second(model, block, source):
        return remote(
            source,
            block_rows(entry_slots, model, me),
            in_send2.at[model, block],
            in_recv2.at[model, me],
            block,
            ex,
        )

    def entry_forward(model, block, source):
        @pl.when(block != me)
        def _():
            entry_second(model, block, source).start()

        @pl.when(block == me)
        def _():
            block_rows(entry_slots, model, me)[...] = source[...]

    def entry_own(model):
        for half in range(halves):
            entry_forward(model, ex * halves + half, placed_at(ex, model, half))

    def entry_relayed(model):
        for peer in reversed(ex_peers):
            for half in range(halves):
                block = peer * halves + half
                held = entry_relay.at[model, block]
                remote(
                    held, held, in_send.at[model, 0, half], in_recv.at[model, block], me, peer
                ).wait_recv()
                entry_forward(model, block, held)

    def entry_pack(model):
        for peer in dp_peers:
            landing = block_rows(entry_slots, model, peer)
            remote(
                landing, landing, in_send2.at[model, peer], in_recv2.at[model, peer], peer, ex
            ).wait_recv()
        rows_ref[model] = jnp.dot(
            gather_ref[...], entry_slots[model], preferred_element_type=jnp.float32
        ).astype(jnp.bfloat16)

    def entry_close():
        for model in range(2):
            for step in range(z - 1):
                for half in range(halves):
                    entry_first(model, step, half).wait_send()
            for peer in dp_peers:
                entry_second(model, peer, entry_relay.at[model, peer]).wait_send()


    def arrival(model, expert, half):
        rows = pl.ds(pl.multiple_of(expert * cap, cap), cap)
        lanes = pl.ds(pl.multiple_of(half * depth, depth), depth)
        return arrived_ref.at[model, rows, lanes]

    def exit_first(model, step):
        return remote(
            block_rows(exit_slots, model, dp_peers[step]),
            exit_relay.at[model, me],
            out_send.at[model, step],
            out_recv.at[model, me],
            dp_peers[step],
            ex,
        )

    def exit_second(model, block, source):
        half = lax.rem(block, halves)
        return remote(
            source,
            arrival(model, ex, half),
            out_send2.at[model, block],
            out_recv2.at[model, ex, half],
            me,
            block // halves,
        )

    def exit_spread(model):
        exit_slots[model] = jnp.dot(
            spread_ref[...], outs[model], preferred_element_type=jnp.float32
        ).astype(jnp.bfloat16)
        for step in range(n - 1):
            exit_first(model, step).start()

    def exit_forward(model, block, source):
        @pl.when(block // halves != ex)
        def _():
            exit_second(model, block, source).start()

        @pl.when(block // halves == ex)
        def _():
            arrival(model, ex, lax.rem(block, halves))[...] = source[...]

    def exit_own(model):
        exit_forward(model, me, block_rows(exit_slots, model, me))

    def exit_relayed(model, block):
        held = exit_relay.at[model, block]
        remote(held, held, out_send.at[model, 0], out_recv.at[model, block], block, ex).wait_recv()
        exit_forward(model, block, held)

    def exit_close(model):
        for peer in ex_peers:
            for half in range(halves):
                landing = arrival(model, peer, half)
                block = peer * halves + half
                remote(
                    landing,
                    landing,
                    out_send2.at[model, block],
                    out_recv2.at[model, peer, half],
                    me,
                    peer,
                ).wait_recv()
                exit_second(model, block, exit_relay.at[model, block]).wait_send()
        for step in range(n - 1):
            exit_first(model, step).wait_send()

    def stats_copy(step):
        return remote(
            stats_ref,
            all_stats.at[me],
            stats_sem.at[0, step],
            stats_sem.at[1, step],
            dp_peers[step],
            ex,
        )


    def bit(stride):
        return lax.rem(me // stride, 2)

    def partner(stride):
        return me + stride * (1 - 2 * bit(stride))

    def tiles(half, u, ref, block, span, held):
        low = bit(1)
        parity = 1 - low if half == 0 else low
        slot = lax.rem(u, 2)
        for q in range(n // 2):
            start = pl.multiple_of((2 * q + parity) * span + block * w, w)
            yield pltpu.make_async_copy(
                ref.at[:, pl.ds(start, w)], held.at[half, slot, q], wsem.at[half, slot, q]
            )

    def fetch(half, u):
        model, block, which = plan.gu_at(u)
        for m, g, ref in ((0, 0, gate0), (0, 1, up0), (1, 0, gate1), (1, 1, up1)):

            @pl.when(plan.is_gu(u) & (model == m) & (which == g))
            def _():
                for copy in tiles(half, u, ref, block, width, wide):
                    copy.start()

        dn_model, dn_block = plan.dn_at(u)
        for m, ref in ((0, down0), (1, down1)):

            @pl.when(plan.is_dn(u) & (dn_model == m))
            def _():
                for copy in tiles(half, u, ref, dn_block, depth, tall):
                    copy.start()

    def arrived(half, u):
        for condition, ref, span, held in (
            (plan.is_gu(u), gate0, width, wide),
            (plan.is_dn(u), down0, depth, tall),
        ):

            @pl.when(condition)
            def _():
                for copy in tiles(half, u, ref, 0, span, held):
                    copy.wait()

    def gu_product(u, half, q):
        model, _, _ = plan.gu_at(u)
        return jnp.dot(
            rows_ref[model],
            wide[half, lax.rem(u, 2), q],
            preferred_element_type=jnp.float32,
        )

    def dn_product(u, half, q):
        model, _ = plan.dn_at(u)
        return jnp.dot(
            hidden[model],
            tall[half, lax.rem(u, 2), q],
            preferred_element_type=jnp.float32,
        )

    def placing(p, u):
        color = lax.rem(u, 2)
        one, two = bit(2**p), bit(2 ** (levels - p))
        mine = one + color * (two - one)
        top = 2 ** (levels - p - 1)

        def place(r, keep):
            value = mine if keep else 1 - mine
            return r * (2 - color) + value * (1 + color * (top - 1))

        return place

    def hop(p, u):
        color = lax.rem(u, 2)
        one, two = partner(2 ** p), partner(2 ** (levels - p) if p else 1)
        return remote(
            sends[p].at[lax.rem(u, send_slots)],
            recvs[p].at[plan.buffer(u)],
            ssem.at[p, lax.rem(u, send_slots)],
            rsem.at[p, plan.buffer(u)],
            one + color * (two - one),
            ex,
        )

    def level_zero(u):
        arrived(0, u)
        slot = lax.rem(u, send_slots)
        for condition, product in ((plan.is_gu(u), gu_product), (plan.is_dn(u), dn_product)):

            @pl.when(condition)
            def _():
                for q in range(n // 2):
                    sends[0][slot, q] = product(u, 0, q).astype(jnp.bfloat16)
                hop(0, u).start()

    def level_one(u):
        arrived(1, u)
        slot, kept, buffer = lax.rem(u, send_slots), lax.rem(u, keep_slots), plan.buffer(u)
        place = placing(1, u)
        for condition, product in ((plan.is_gu(u), gu_product), (plan.is_dn(u), dn_product)):

            @pl.when(condition)
            def _():
                hop(0, u).wait_recv()
                for keep in (False, True):
                    for r in range(n // 4):
                        at = place(r, keep)
                        total = product(u, 1, at) + recvs[0][buffer, at].astype(jnp.float32)
                        if keep:
                            keeps[0][kept, r] = total.astype(jnp.bfloat16)
                        else:
                            sends[1][slot, r] = total.astype(jnp.bfloat16)
                    if not keep:
                        hop(1, u).start()

    def level(p, u):
        slot, kept, buffer = lax.rem(u, send_slots), lax.rem(u, keep_slots), plan.buffer(u)
        place = placing(p, u)

        @pl.when(plan.is_gu(u) | plan.is_dn(u))
        def _():
            hop(p - 1, u).wait_recv()
            for keep in (False, True):
                for r in range(n // 2 ** (p + 1)):
                    at = place(r, keep)
                    total = keeps[p - 2][kept, at].astype(jnp.float32) + recvs[p - 1][
                        buffer, at
                    ].astype(jnp.float32)
                    if keep:
                        keeps[p - 1][kept, r] = total.astype(jnp.bfloat16)
                    else:
                        sends[p][slot, r] = total.astype(jnp.bfloat16)
                if not keep:
                    hop(p, u).start()

    def finish(u):
        kept, buffer = lax.rem(u, keep_slots), plan.buffer(u)

        def total():
            return keeps[-1][kept, 0].astype(jnp.float32) + recvs[-1][buffer, 0].astype(jnp.float32)

        @pl.when(plan.is_gu(u) | plan.is_dn(u))
        def _():
            hop(levels - 1, u).wait_recv()

        model, block, which = plan.gu_at(u)

        @pl.when(plan.is_gu(u) & (which == 0))
        def _():
            gated[...] = total()

        @pl.when(plan.is_gu(u) & (which == 1))
        def _():
            value = gated[...]
            hidden[model, :, pl.ds(pl.multiple_of(block * w, w), w)] = (
                value / (1.0 + jnp.exp(-value)) * total()
            ).astype(jnp.bfloat16)

        dn_model, dn_block = plan.dn_at(u)

        @pl.when(plan.is_dn(u))
        def _():
            outs[dn_model, :, pl.ds(pl.multiple_of(dn_block * w, w), w)] = total().astype(
                jnp.bfloat16
            )

        @pl.when(plan.is_gu(u) | plan.is_dn(u))
        def _():
            for p in range(levels):
                hop(p, u).wait_send()

    fetch(0, jnp.int32(0))
    greet([(me, peer) for peer in ex_peers] + [(peer, ex) for peer in dp_peers])
    for model in range(2):
        for step in range(z - 1):
            for half in range(halves):
                entry_first(model, step, half).start()
        if model == 0:
            entry_own(0)
    entry_relayed(0)
    entry_pack(0)
    entry_own(1)
    for step in range(n - 1):
        stats_copy(step).start()
    all_stats[me] = stats_ref[...]

    def step(t, carry):
        fetch(0, t + 1)
        fetch(1, t)
        finish(t - lags[levels])
        for p in range(levels - 1, 1, -1):
            level(p, t - lags[p])
        level_one(t - lags[1])

        @pl.when(t == plan.gu)
        def _():
            entry_pack(1)

        level_zero(t)

        @pl.when(t == 2)
        def _():
            entry_relayed(1)

        @pl.when(t == plan.leave0)
        def _():
            exit_spread(0)
            exit_own(0)

        for index in range(plan.each):
            place = (t - plan.leave0 - 1) * plan.each + index + 1

            @pl.when((place > 0) & (place < n))
            def _():
                exit_relayed(0, lax.rem(me + n - place, n))

        return carry

    lax.fori_loop(0, plan.steps, step, 0)
    exit_spread(1)
    exit_own(1)
    for peer in reversed(dp_peers):
        exit_relayed(1, peer)
    entry_close()
    for model in range(2):
        exit_close(model)
    for step in range(n - 1):
        stats_copy(step).wait()


def experts(n, z, cap, chunk, collective, placed, gather, spread, stats, weights):
    (gate0, up0, down0), (gate1, up1, down1) = weights
    depth, width = gate0.shape[0], down0.shape[0]
    w = depth // 2
    plan = Plan(n, width // w, depth // w)
    levels, halves = plan.levels, n // z
    if 2**levels != n or levels < 2 or halves * z != n:
        raise ValueError("mesh size")
    send_slots, keep_slots = plan.lags[-1] + 1, 4
    bf = jnp.bfloat16
    parts = [n // 2 ** (p + 1) for p in range(levels)]
    flops = 2 * chunk * 3 * depth * n * width * 2
    dma = pltpu.SemaphoreType.DMA
    return pl.pallas_call(
        functools.partial(expert_kernel, n, z, plan),
        out_shape=(
            jax.ShapeDtypeStruct((2, z * cap, halves * depth), bf),
            jax.ShapeDtypeStruct((n,) + stats.shape, stats.dtype),
        ),
        in_specs=[VMEM] * 4 + [ANY] * 6,
        out_specs=(VMEM,) * 2,
        scratch_shapes=[pltpu.VMEM((send_slots, part, chunk, w), bf) for part in parts]
        + [pltpu.VMEM((plan.units, part, chunk, w), bf) for part in parts]
        + [pltpu.VMEM((keep_slots, part, chunk, w), bf) for part in parts[1:]]
        + [
            pltpu.VMEM((2, 2, n // 2, depth, w), bf),
            pltpu.VMEM((2, 2, n // 2, width, w), bf),
            pltpu.VMEM((2, chunk, width), bf),
            pltpu.VMEM((chunk, w), jnp.float32),
            dma((2, 2, n // 2)),
            dma((levels, send_slots)),
            dma((levels, plan.units)),
            pltpu.VMEM((2, n, cap, depth), bf),
            pltpu.VMEM((2, n * cap, depth), bf),
            pltpu.VMEM((2, chunk, depth), bf),
            pltpu.VMEM((2, chunk, depth), bf),
            pltpu.VMEM((2, n * cap, depth), bf),
            pltpu.VMEM((2, n, cap, depth), bf),
            dma((2, n - 1)),
            dma((2, z - 1, halves)),
            dma((2, n)),
            dma((2, n)),
            dma((2, n)),
            dma((2, n - 1)),
            dma((2, n)),
            dma((2, n)),
            dma((2, z, halves)),
        ],
        compiler_params=pltpu.CompilerParams(
            collective_id=collective, has_side_effects=True, vmem_limit_bytes=VMEM_LIMIT
        ),
        cost_estimate=pl.CostEstimate(
            flops=flops, bytes_accessed=12 * depth * n * width, transcendentals=0
        ),
        name=f"experts_{chunk}",
    )(placed, gather, spread, stats, gate0, up0, down0, gate1, up1, down1)


def per_device(
    policy_hidden,
    reference_hidden,
    policy_norm_gain,
    reference_norm_gain,
    policy_router,
    reference_router,
    policy_gate,
    policy_up,
    policy_down,
    reference_gate,
    reference_up,
    reference_down,
    expert_ids,
    lengths,
):
    n, z = lax.axis_size("dp"), lax.axis_size("expert")
    ex = lax.axis_index("expert")
    tokens, features = policy_hidden.shape
    routes = expert_ids.shape[1]
    cap = 3 * tokens // z
    depth = policy_gate.shape[1]
    token_total = float(tokens * n)
    f32, bf = jnp.float32, jnp.bfloat16

    live = (jnp.arange(SEG, dtype=jnp.int32)[None, :] < lengths[:, None]).reshape(-1)
    live_f = live.astype(f32)
    flat_ids = expert_ids.reshape(-1)
    flat_live = jnp.repeat(live, routes)
    choice = flat_ids[:, None] == jnp.arange(z, dtype=jnp.int32)[None, :]
    onehot = (choice & flat_live[:, None]).astype(bf)
    order = jnp.arange(tokens * routes, dtype=jnp.int32)
    earlier = (order[None, :] < order[:, None]).astype(bf)
    before = jnp.dot(earlier, onehot, preferred_element_type=f32)
    pos = jnp.sum(before * choice.astype(f32), axis=1).astype(jnp.int32)
    counts = jnp.sum(onehot.astype(f32), axis=0)
    counts_tile = jnp.pad(counts[None, :], ((0, 7), (0, 128 - z)))

    def router_terms(hidden, gain, router):
        values = hidden.astype(f32)
        logits = lax.dot_general(
            router, values * gain, (((0,), (1,)), ((), ())), precision=lax.Precision.HIGHEST
        )
        return jnp.concatenate((logits, jnp.sum(values * values, axis=1)[None, :]), axis=0)

    terms = jnp.concatenate(
        (
            router_terms(policy_hidden, policy_norm_gain, policy_router),
            router_terms(reference_hidden, reference_norm_gain, reference_router),
        ),
        axis=0,
    )
    terms = jnp.pad(terms, ((0, -terms.shape[0] % 8), (0, 0)))
    all_terms, all_counts = small_exchange(n, z, terms, counts_tile)
    terms = jnp.sum(all_terms, axis=0)
    block_counts = all_counts[:, 0, :z].astype(jnp.int32)

    def model_terms(base, hidden, gain):
        scale = lax.rsqrt(terms[base + z] / (n * depth) + EPSILON)
        logits = terms[base : base + z] * scale[None, :]
        rows = (hidden.astype(f32) * gain * scale[:, None]).astype(bf)
        return logits, rows

    policy_logits, policy_rows = model_terms(0, policy_hidden, policy_norm_gain)
    reference_logits, reference_rows = model_terms(z + 1, reference_hidden, reference_norm_gain)

    totals = jnp.sum(block_counts, axis=0)
    mine = lax.dynamic_slice_in_dim(block_counts, ex, 1, axis=1)[:, 0]
    first = jnp.cumsum(mine) - mine
    stacked = jnp.concatenate((policy_rows, reference_rows), axis=1)
    weights = (
        (policy_gate[0], policy_up[0], policy_down[0]),
        (reference_gate[0], reference_up[0], reference_down[0]),
    )

    policy_logprob = jax.nn.log_softmax(policy_logits, axis=0)
    reference_logprob = jax.nn.log_softmax(reference_logits, axis=0)
    policy_prob = jnp.exp(policy_logprob)
    token_kl = jnp.sum(policy_prob * (policy_logprob - reference_logprob), axis=0) * live_f
    probsum = jnp.sum(policy_prob * live_f[None, :], axis=1)
    stats = jnp.concatenate((probsum, jnp.sum(token_kl)[None]))
    stats_tile = jnp.pad(stats[None, :], ((0, 7), (0, 128 - z - 1)))

    def pair_gates(logits):
        matches = expert_ids[:, :, None] == jnp.arange(z, dtype=jnp.int32)[None, None, :]
        chosen = jnp.sum(jnp.where(matches, logits.T[:, None, :], 0.0), axis=2)
        return jax.nn.softmax(chosen, axis=1)

    gates = (pair_gates(policy_logits), pair_gates(reference_logits))

    def layer(held, chunk, collective, single):
        target = jnp.where(flat_live, flat_ids * held + pos, -1).reshape(tokens, routes)
        slot = jnp.arange(z * held, dtype=jnp.int32)
        select = sum(slot[:, None] == target[:, k][None, :] for k in range(routes)).astype(bf)
        placed = jnp.dot(select, stacked, preferred_element_type=f32).astype(bf)
        within = jnp.arange(held, dtype=jnp.int32)
        packed = jnp.where(
            within[None, :] < mine[:, None], first[:, None] + within[None, :], -1
        ).reshape(-1)

        def one_chunk(index):
            wanted = index * chunk + jnp.arange(chunk, dtype=jnp.int32)
            gather = (wanted[:, None] == packed[None, :]).astype(bf)
            spread = (packed[:, None] == wanted[None, :]).astype(bf)
            return experts(n, z, held, chunk, collective, placed, gather, spread, stats_tile, weights)

        def body(index, carry):
            arrived, all_stats = one_chunk(index)
            return carry[0] + arrived, all_stats

        if single:
            arrived, all_stats = one_chunk(0)
        else:
            zeros = (
                jnp.zeros((2, z * held, features), bf),
                jnp.zeros((n,) + stats_tile.shape, f32),
            )
            arrived, all_stats = lax.fori_loop(0, (need + chunk - 1) // chunk, body, zeros)

        def combine(model):
            total = 0.0
            for k in range(routes):
                pick = (target[:, k][:, None] == slot[None, :]).astype(bf)
                picked = jnp.dot(pick, arrived[model], preferred_element_type=f32)
                total = total + picked * gates[model][:, k : k + 1]
            return (total * live_f[:, None]).astype(bf)

        return combine(0), combine(1), all_stats

    need, need_held = jnp.max(totals), jnp.max(block_counts)
    sizes = []
    for part, rows in SIZES:
        size = (-(-part * cap // 6 // 16) * 16, -(-rows * n * cap // 48 // 16) * 16)
        if size not in sizes:
            sizes.append(size)
    branch = sum(
        ((need > chunk) | (need_held > held)).astype(jnp.int32) for held, chunk in sizes
    )
    branches = [
        functools.partial(layer, held, chunk, 1 + index, True)
        for index, (held, chunk) in enumerate(sizes)
    ] + [functools.partial(layer, *sizes[-1], len(sizes), False)]
    policy_mixture, reference_mixture, all_stats = lax.switch(branch, branches)

    stats = jnp.sum(all_stats[:, 0, :], axis=0)
    balance = z * jnp.sum(
        totals.astype(f32) / (routes * token_total) * stats[:z] / token_total
    )
    loss = KL_WEIGHT * stats[z] / token_total + BALANCE_WEIGHT * balance
    return (policy_mixture, reference_mixture, token_kl, loss)


def solution(mesh):
    in_specs = (
        P("dp", "expert"),
        P("dp", "expert"),
        P("expert"),
        P("expert"),
        P("expert", None),
        P("expert", None),
        P("expert", "dp", None),
        P("expert", "dp", None),
        P("expert", "dp", None),
        P("expert", "dp", None),
        P("expert", "dp", None),
        P("expert", "dp", None),
        P("dp", None),
        P("dp"),
    )
    out_specs = (P("dp", "expert"), P("dp", "expert"), P("dp"), P())
    return jax.shard_map(
        per_device, mesh=mesh, in_specs=in_specs, out_specs=out_specs, check_vma=False
    )
```

```python
import functools

import jax
import jax.numpy as jnp
from jax import lax
from jax.experimental import pallas as pl
from jax.experimental.pallas import tpu as pltpu
from jax.sharding import PartitionSpec as P

D = 4096
SEG = 32

EPSILON = 1e-05
KL_WEIGHT = 1.0
BALANCE_WEIGHT = 0.5
SIZES = ((4, 18), (5, 19), (6, 20))

MESH = pl.DeviceIdType.MESH
VMEM = pl.BlockSpec(memory_space=pltpu.VMEM)
ANY = pl.BlockSpec(memory_space=pl.ANY)
VMEM_LIMIT = 67043328


def remote(src, dst, send_sem, recv_sem, dp, expert):
    return pltpu.make_async_remote_copy(
        src_ref=src,
        dst_ref=dst,
        send_sem=send_sem,
        recv_sem=recv_sem,
        device_id=(dp, expert),
        device_id_type=MESH,
    )


def greet(peers):
    barrier = pltpu.get_barrier_semaphore()
    for peer in peers:
        pl.semaphore_signal(barrier, inc=1, device_id=peer, device_id_type=MESH)
    pl.semaphore_wait(barrier, len(peers))


def around(index, size):
    return [lax.rem(index + step, size) for step in range(1, size)]


def column(row):
    size = row.shape[1]
    across = lax.broadcasted_iota(jnp.int32, (size, size), 0)
    along = lax.broadcasted_iota(jnp.int32, (size, size), 1)
    return jnp.sum(jnp.where(across == along, row, 0.0), axis=1, keepdims=True)


def router_kernel(
    n,
    z,
    routes,
    hidden0,
    hidden1,
    gain0,
    gain1,
    router0,
    router1,
    ids_ref,
    live_ref,
    counts_ref,
    rows_ref,
    gates_ref,
    stats_ref,
    all_counts,
    terms,
    all_terms,
    sems,
):
    dp, ex = lax.axis_index("dp"), lax.axis_index("expert")
    ex_peers, dp_peers = around(ex, z), around(dp, n)
    features = hidden0.shape[1]
    lead = terms.shape[0] // 2 - 8
    exact = lax.Precision.HIGHEST
    along = (((1,), (1,)), ((), ()))
    models = ((hidden0, gain0, router0), (hidden1, gain1, router1))
    terms[...] = jnp.zeros_like(terms)
    for model, (hidden, gain, router) in enumerate(models):
        base = model * (lead + 8)
        values = hidden[...].astype(jnp.float32)
        terms[base : base + z] = lax.dot_general(
            router[...],
            values * gain[...],
            along,
            precision=exact,
            preferred_element_type=jnp.float32,
        )
        terms[base + lead : base + lead + 8] = lax.dot_general(
            jnp.ones((8, features), jnp.float32),
            values * values,
            along,
            precision=exact,
            preferred_element_type=jnp.float32,
        )
    greet([(dp, peer) for peer in ex_peers] + [(peer, ex) for peer in dp_peers])
    copies = []
    for step, peer in enumerate(ex_peers):
        at = n - 1 + step
        copies.append(
            remote(terms, all_terms.at[ex], sems.at[0, at], sems.at[1, at], dp, peer)
        )
    for step, peer in enumerate(dp_peers):
        copies.append(
            remote(counts_ref, all_counts.at[dp], sems.at[0, step], sems.at[1, step], peer, ex)
        )
    for copy in copies:
        copy.start()
    all_counts[dp] = counts_ref[...]
    all_terms[ex] = terms[...]
    for copy in copies:
        copy.wait()
    total = all_terms[0]
    for index in range(1, z):
        total = total + all_terms[index]
    live = live_ref[...]
    logprobs = []
    for model, (hidden, gain, router) in enumerate(models):
        base = model * (lead + 8)
        squares = total[base + lead : base + lead + 1]
        scale = lax.rsqrt(squares / (z * features) + EPSILON)
        logits = total[base : base + z] * scale
        rows_ref[:, model * features : (model + 1) * features] = (
            hidden[...].astype(jnp.float32) * gain[...] * column(scale)
        ).astype(jnp.bfloat16)
        chosen = []
        for k in range(routes):
            ids = ids_ref[k : k + 1, :]
            pick = jnp.zeros_like(scale)
            for expert in range(z):
                pick = pick + jnp.where(ids == expert, logits[expert : expert + 1], 0.0)
            chosen.append(pick)
        most = chosen[0]
        for pick in chosen[1:]:
            most = jnp.maximum(most, pick)
        raised = [jnp.exp(pick - most) for pick in chosen]
        below = raised[0]
        for pick in raised[1:]:
            below = below + pick
        for k in range(routes):
            at = model * routes + k
            gates_ref[:, at : at + 1] = column(raised[k] / below * live)
        shifted = logits - jnp.max(logits, axis=0, keepdims=True)
        logprobs.append(shifted - jnp.log(jnp.sum(jnp.exp(shifted), axis=0, keepdims=True)))
    prob = jnp.exp(logprobs[0])
    stats_ref[...] = jnp.zeros_like(stats_ref)
    stats_ref[0:z] = prob * live
    stats_ref[lead : lead + 1] = (
        jnp.sum(prob * (logprobs[0] - logprobs[1]), axis=0, keepdims=True) * live
    )


def router_terms(n, z, hiddens, gains, routers, ids, live, counts):
    tokens, features = hiddens[0].shape
    routes = ids.shape[0]
    lead = -(-z // 8) * 8
    f32 = jnp.float32
    return pl.pallas_call(
        functools.partial(router_kernel, n, z, routes),
        out_shape=(
            jax.ShapeDtypeStruct((tokens, 2 * features), jnp.bfloat16),
            jax.ShapeDtypeStruct((tokens, 2 * routes), f32),
            jax.ShapeDtypeStruct((lead + 8, tokens), f32),
            jax.ShapeDtypeStruct((n,) + counts.shape, counts.dtype),
        ),
        in_specs=[VMEM] * 9,
        out_specs=(VMEM,) * 4,
        scratch_shapes=[
            pltpu.VMEM((2 * (lead + 8), tokens), f32),
            pltpu.VMEM((z, 2 * (lead + 8), tokens), f32),
            pltpu.SemaphoreType.DMA((2, n + z - 2)),
        ],
        compiler_params=pltpu.CompilerParams(collective_id=0, has_side_effects=True),
        name="router_terms",
    )(*hiddens, *gains, *routers, ids, live, counts)


class Plan:
    def __init__(self, n, blocks_up, blocks_down):
        self.levels = n.bit_length() - 1
        self.lags = [0] + [2 * p - 1 for p in range(1, self.levels + 1)]
        last = self.lags[-1]
        self.gu = 2 * blocks_up
        self.dn = blocks_down
        self.down0 = self.gu - 1 + last
        self.rest = self.down0 + self.dn
        self.end = 2 * self.gu + self.dn
        self.down1 = self.end - 1 + last
        self.ids = self.down1 + self.dn
        self.units = self.end + self.dn
        self.steps = self.ids + last
        self.leave0 = max(self.rest - 1 + last, self.end - 1 + self.lags[-2])
        self.each = -(-n // (self.steps - self.leave0 - 1))

    def is_gu(self, u):
        return ((u >= 0) & (u < self.down0)) | ((u >= self.rest) & (u < self.end))

    def is_dn(self, u):
        return ((u >= self.down0) & (u < self.rest)) | ((u >= self.down1) & (u < self.ids))

    def gu_at(self, u):
        index = jnp.where(u < self.down0, u, u - self.dn)
        inner = lax.rem(index, self.gu)
        return index // self.gu, inner // 2, lax.rem(inner, 2)

    def dn_at(self, u):
        late = u >= self.rest
        return jnp.where(late, 1, 0), jnp.where(late, u - self.down1, u - self.down0)

    def buffer(self, u):
        return jnp.where(u < self.end, u, u - (self.down1 - self.end))


def expert_kernel(
    n,
    z,
    plan,
    placed,
    gather_ref,
    spread_ref,
    stats_ref,
    picks_ref,
    gates_ref,
    gate0,
    up0,
    down0,
    gate1,
    up1,
    down1,
    mixed_ref,
    all_stats,
    *scratch,
):
    levels, lags = plan.levels, plan.lags
    sends, recvs = scratch[:levels], scratch[levels : 2 * levels]
    keeps = scratch[2 * levels : 3 * levels - 1]
    (
        wide,
        tall,
        hidden,
        gated,
        wsem,
        ssem,
        rsem,
        entry_relay,
        entry_slots,
        rows_ref,
        outs,
        exit_slots,
        exit_relay,
        stats_sem,
        in_send,
        in_recv,
        in_send2,
        in_recv2,
        out_send,
        out_recv,
        out_send2,
        out_recv2,
        arrived_ref,
    ) = scratch[3 * levels - 1 :]
    me, ex = lax.axis_index("dp"), lax.axis_index("expert")
    w = wide.shape[-1]
    depth, width = gate0.shape[0], down0.shape[0]
    send_slots, keep_slots = sends[0].shape[0], keeps[0].shape[0]
    halves, cap = n // z, entry_relay.shape[2]
    ex_peers, dp_peers = around(ex, z), around(me, n)

    def block_rows(ref, model, block):
        return ref.at[model, pl.ds(pl.multiple_of(block * cap, cap), cap), :]


    def placed_at(expert, model, half):
        rows = pl.ds(pl.multiple_of(expert * cap, cap), cap)
        return placed.at[rows, pl.ds((model * halves + half) * depth, depth)]

    def entry_first(model, step, half):
        return remote(
            placed_at(ex_peers[step], model, half),
            entry_relay.at[model, ex * halves + half],
            in_send.at[model, step, half],
            in_recv.at[model, ex * halves + half],
            me,
            ex_peers[step],
        )

    def entry_second(model, block, source):
        return remote(
            source,
            block_rows(entry_slots, model, me),
            in_send2.at[model, block],
            in_recv2.at[model, me],
            block,
            ex,
        )

    def entry_forward(model, block, source):
        @pl.when(block != me)
        def _():
            entry_second(model, block, source).start()

        @pl.when(block == me)
        def _():
            block_rows(entry_slots, model, me)[...] = source[...]

    def entry_own(model):
        for half in range(halves):
            entry_forward(model, ex * halves + half, placed_at(ex, model, half))

    def entry_relayed(model):
        for peer in reversed(ex_peers):
            for half in range(halves):
                block = peer * halves + half
                held = entry_relay.at[model, block]
                remote(
                    held, held, in_send.at[model, 0, half], in_recv.at[model, block], me, peer
                ).wait_recv()
                entry_forward(model, block, held)

    def entry_pack(model):
        for peer in dp_peers:
            landing = block_rows(entry_slots, model, peer)
            remote(
                landing, landing, in_send2.at[model, peer], in_recv2.at[model, peer], peer, ex
            ).wait_recv()
        rows_ref[model] = jnp.dot(
            gather_ref[...], entry_slots[model], preferred_element_type=jnp.float32
        ).astype(jnp.bfloat16)

    def entry_close():
        for model in range(2):
            for step in range(z - 1):
                for half in range(halves):
                    entry_first(model, step, half).wait_send()
            for peer in dp_peers:
                entry_second(model, peer, entry_relay.at[model, peer]).wait_send()


    def arrival(model, expert, half):
        rows = pl.ds(pl.multiple_of(expert * cap, cap), cap)
        lanes = pl.ds(pl.multiple_of(half * depth, depth), depth)
        return arrived_ref.at[model, rows, lanes]

    def exit_first(model, step):
        return remote(
            block_rows(exit_slots, model, dp_peers[step]),
            exit_relay.at[model, me],
            out_send.at[model, step],
            out_recv.at[model, me],
            dp_peers[step],
            ex,
        )

    def exit_second(model, block, source):
        half = lax.rem(block, halves)
        return remote(
            source,
            arrival(model, ex, half),
            out_send2.at[model, block],
            out_recv2.at[model, ex, half],
            me,
            block // halves,
        )

    def exit_spread(model):
        exit_slots[model] = jnp.dot(
            spread_ref[...], outs[model], preferred_element_type=jnp.float32
        ).astype(jnp.bfloat16)
        for step in range(n - 1):
            exit_first(model, step).start()

    def exit_forward(model, block, source):
        @pl.when(block // halves != ex)
        def _():
            exit_second(model, block, source).start()

        @pl.when(block // halves == ex)
        def _():
            arrival(model, ex, lax.rem(block, halves))[...] = source[...]

    def exit_own(model):
        exit_forward(model, me, block_rows(exit_slots, model, me))

    def exit_relayed(model, block):
        held = exit_relay.at[model, block]
        remote(held, held, out_send.at[model, 0], out_recv.at[model, block], block, ex).wait_recv()
        exit_forward(model, block, held)

    def exit_close(model):
        for peer in ex_peers:
            for half in range(halves):
                landing = arrival(model, peer, half)
                block = peer * halves + half
                remote(
                    landing,
                    landing,
                    out_send2.at[model, block],
                    out_recv2.at[model, peer, half],
                    me,
                    peer,
                ).wait_recv()
                exit_second(model, block, exit_relay.at[model, block]).wait_send()
        for step in range(n - 1):
            exit_first(model, step).wait_send()
        routes = picks_ref.shape[0]
        total = 0.0
        for k in range(routes):
            at = model * routes + k
            total = total + gates_ref[:, at : at + 1] * jnp.dot(
                picks_ref[k], arrived_ref[model], preferred_element_type=jnp.float32
            )
        mixed_ref[model] = total

    def stats_copy(step):
        return remote(
            stats_ref,
            all_stats.at[me],
            stats_sem.at[0, step],
            stats_sem.at[1, step],
            dp_peers[step],
            ex,
        )


    def bit(stride):
        return lax.rem(me // stride, 2)

    def partner(stride):
        return me + stride * (1 - 2 * bit(stride))

    def tiles(half, u, ref, block, span, held):
        low = bit(1)
        parity = 1 - low if half == 0 else low
        slot = lax.rem(u, 2)
        for q in range(n // 2):
            start = pl.multiple_of((2 * q + parity) * span + block * w, w)
            yield pltpu.make_async_copy(
                ref.at[:, pl.ds(start, w)], held.at[half, slot, q], wsem.at[half, slot, q]
            )

    def fetch(half, u):
        model, block, which = plan.gu_at(u)
        for m, g, ref in ((0, 0, gate0), (0, 1, up0), (1, 0, gate1), (1, 1, up1)):

            @pl.when(plan.is_gu(u) & (model == m) & (which == g))
            def _():
                for copy in tiles(half, u, ref, block, width, wide):
                    copy.start()

        dn_model, dn_block = plan.dn_at(u)
        for m, ref in ((0, down0), (1, down1)):

            @pl.when(plan.is_dn(u) & (dn_model == m))
            def _():
                for copy in tiles(half, u, ref, dn_block, depth, tall):
                    copy.start()

    def arrived(half, u):
        for condition, ref, span, held in (
            (plan.is_gu(u), gate0, width, wide),
            (plan.is_dn(u), down0, depth, tall),
        ):

            @pl.when(condition)
            def _():
                for copy in tiles(half, u, ref, 0, span, held):
                    copy.wait()

    def gu_product(u, half, q):
        model, _, _ = plan.gu_at(u)
        return jnp.dot(
            rows_ref[model],
            wide[half, lax.rem(u, 2), q],
            preferred_element_type=jnp.float32,
        )

    def dn_product(u, half, q):
        model, _ = plan.dn_at(u)
        return jnp.dot(
            hidden[model],
            tall[half, lax.rem(u, 2), q],
            preferred_element_type=jnp.float32,
        )

    def placing(p, u):
        color = lax.rem(u, 2)
        one, two = bit(2**p), bit(2 ** (levels - p))
        mine = one + color * (two - one)
        top = 2 ** (levels - p - 1)

        def place(r, keep):
            value = mine if keep else 1 - mine
            return r * (2 - color) + value * (1 + color * (top - 1))

        return place

    def hop(p, u):
        color = lax.rem(u, 2)
        one, two = partner(2 ** p), partner(2 ** (levels - p) if p else 1)
        return remote(
            sends[p].at[lax.rem(u, send_slots)],
            recvs[p].at[plan.buffer(u)],
            ssem.at[p, lax.rem(u, send_slots)],
            rsem.at[p, plan.buffer(u)],
            one + color * (two - one),
            ex,
        )

    def level_zero(u):
        arrived(0, u)
        slot = lax.rem(u, send_slots)
        for condition, product in ((plan.is_gu(u), gu_product), (plan.is_dn(u), dn_product)):

            @pl.when(condition)
            def _():
                for q in range(n // 2):
                    sends[0][slot, q] = product(u, 0, q).astype(jnp.bfloat16)
                hop(0, u).start()

    def level_one(u):
        arrived(1, u)
        slot, kept, buffer = lax.rem(u, send_slots), lax.rem(u, keep_slots), plan.buffer(u)
        place = placing(1, u)
        for condition, product in ((plan.is_gu(u), gu_product), (plan.is_dn(u), dn_product)):

            @pl.when(condition)
            def _():
                hop(0, u).wait_recv()
                for keep in (False, True):
                    for r in range(n // 4):
                        at = place(r, keep)
                        total = product(u, 1, at) + recvs[0][buffer, at].astype(jnp.float32)
                        if keep:
                            keeps[0][kept, r] = total.astype(jnp.bfloat16)
                        else:
                            sends[1][slot, r] = total.astype(jnp.bfloat16)
                    if not keep:
                        hop(1, u).start()

    def level(p, u):
        slot, kept, buffer = lax.rem(u, send_slots), lax.rem(u, keep_slots), plan.buffer(u)
        place = placing(p, u)

        @pl.when(plan.is_gu(u) | plan.is_dn(u))
        def _():
            hop(p - 1, u).wait_recv()
            for keep in (False, True):
                for r in range(n // 2 ** (p + 1)):
                    at = place(r, keep)
                    total = keeps[p - 2][kept, at].astype(jnp.float32) + recvs[p - 1][
                        buffer, at
                    ].astype(jnp.float32)
                    if keep:
                        keeps[p - 1][kept, r] = total.astype(jnp.bfloat16)
                    else:
                        sends[p][slot, r] = total.astype(jnp.bfloat16)
                if not keep:
                    hop(p, u).start()

    def finish(u):
        kept, buffer = lax.rem(u, keep_slots), plan.buffer(u)

        def total():
            return keeps[-1][kept, 0].astype(jnp.float32) + recvs[-1][buffer, 0].astype(jnp.float32)

        @pl.when(plan.is_gu(u) | plan.is_dn(u))
        def _():
            hop(levels - 1, u).wait_recv()

        model, block, which = plan.gu_at(u)

        @pl.when(plan.is_gu(u) & (which == 0))
        def _():
            gated[...] = total()

        @pl.when(plan.is_gu(u) & (which == 1))
        def _():
            value = gated[...]
            hidden[model, :, pl.ds(pl.multiple_of(block * w, w), w)] = (
                value / (1.0 + jnp.exp(-value)) * total()
            ).astype(jnp.bfloat16)

        dn_model, dn_block = plan.dn_at(u)

        @pl.when(plan.is_dn(u))
        def _():
            outs[dn_model, :, pl.ds(pl.multiple_of(dn_block * w, w), w)] = total().astype(
                jnp.bfloat16
            )

        @pl.when(plan.is_gu(u) | plan.is_dn(u))
        def _():
            for p in range(levels):
                hop(p, u).wait_send()

    fetch(0, jnp.int32(0))
    greet([(me, peer) for peer in ex_peers] + [(peer, ex) for peer in dp_peers])
    for model in range(2):
        for step in range(z - 1):
            for half in range(halves):
                entry_first(model, step, half).start()
        if model == 0:
            entry_own(0)
    entry_relayed(0)
    entry_pack(0)
    entry_own(1)
    for step in range(n - 1):
        stats_copy(step).start()
    all_stats[me] = stats_ref[...]

    def step(t, carry):
        fetch(0, t + 1)
        fetch(1, t)
        finish(t - lags[levels])
        for p in range(levels - 1, 1, -1):
            level(p, t - lags[p])
        level_one(t - lags[1])

        @pl.when(t == plan.gu)
        def _():
            entry_pack(1)

        level_zero(t)

        @pl.when(t == 2)
        def _():
            entry_relayed(1)

        @pl.when(t == plan.leave0)
        def _():
            exit_spread(0)
            exit_own(0)

        for index in range(plan.each):
            place = (t - plan.leave0 - 1) * plan.each + index + 1

            @pl.when((place > 0) & (place < n))
            def _():
                exit_relayed(0, lax.rem(me + n - place, n))

        return carry

    lax.fori_loop(0, plan.steps, step, 0)
    exit_spread(1)
    exit_own(1)
    for peer in reversed(dp_peers):
        exit_relayed(1, peer)
    entry_close()
    for model in range(2):
        exit_close(model)
    for step in range(n - 1):
        stats_copy(step).wait()


def experts(n, z, cap, chunk, collective, placed, gather, spread, stats, picks, gates, weights):
    (gate0, up0, down0), (gate1, up1, down1) = weights
    depth, width = gate0.shape[0], down0.shape[0]
    w = depth // 2
    plan = Plan(n, width // w, depth // w)
    levels, halves = plan.levels, n // z
    if 2**levels != n or levels < 2 or halves * z != n:
        raise ValueError("mesh size")
    send_slots, keep_slots = plan.lags[-1] + 1, 4
    bf = jnp.bfloat16
    parts = [n // 2 ** (p + 1) for p in range(levels)]
    flops = 2 * chunk * 3 * depth * n * width * 2
    dma = pltpu.SemaphoreType.DMA
    return pl.pallas_call(
        functools.partial(expert_kernel, n, z, plan),
        out_shape=(
            jax.ShapeDtypeStruct((2, gates.shape[0], halves * depth), jnp.float32),
            jax.ShapeDtypeStruct((n,) + stats.shape, stats.dtype),
        ),
        in_specs=[VMEM] * 6 + [ANY] * 6,
        out_specs=(VMEM,) * 2,
        scratch_shapes=[pltpu.VMEM((send_slots, part, chunk, w), bf) for part in parts]
        + [pltpu.VMEM((plan.units, part, chunk, w), bf) for part in parts]
        + [pltpu.VMEM((keep_slots, part, chunk, w), bf) for part in parts[1:]]
        + [
            pltpu.VMEM((2, 2, n // 2, depth, w), bf),
            pltpu.VMEM((2, 2, n // 2, width, w), bf),
            pltpu.VMEM((2, chunk, width), bf),
            pltpu.VMEM((chunk, w), jnp.float32),
            dma((2, 2, n // 2)),
            dma((levels, send_slots)),
            dma((levels, plan.units)),
            pltpu.VMEM((2, n, cap, depth), bf),
            pltpu.VMEM((2, n * cap, depth), bf),
            pltpu.VMEM((2, chunk, depth), bf),
            pltpu.VMEM((2, chunk, depth), bf),
            pltpu.VMEM((2, n * cap, depth), bf),
            pltpu.VMEM((2, n, cap, depth), bf),
            dma((2, n - 1)),
            dma((2, z - 1, halves)),
            dma((2, n)),
            dma((2, n)),
            dma((2, n)),
            dma((2, n - 1)),
            dma((2, n)),
            dma((2, n)),
            dma((2, z, halves)),
            pltpu.VMEM((2, z * cap, halves * depth), bf),
        ],
        compiler_params=pltpu.CompilerParams(
            collective_id=collective, has_side_effects=True, vmem_limit_bytes=VMEM_LIMIT
        ),
        cost_estimate=pl.CostEstimate(
            flops=flops, bytes_accessed=12 * depth * n * width, transcendentals=0
        ),
        name=f"experts_{chunk}",
    )(placed, gather, spread, stats, picks, gates, gate0, up0, down0, gate1, up1, down1)


def per_device(
    policy_hidden,
    reference_hidden,
    policy_norm_gain,
    reference_norm_gain,
    policy_router,
    reference_router,
    policy_gate,
    policy_up,
    policy_down,
    reference_gate,
    reference_up,
    reference_down,
    expert_ids,
    lengths,
):
    n, z = lax.axis_size("dp"), lax.axis_size("expert")
    ex = lax.axis_index("expert")
    tokens, features = policy_hidden.shape
    routes = expert_ids.shape[1]
    cap = 3 * tokens // z
    depth = policy_gate.shape[1]
    token_total = float(tokens * n)
    f32, bf = jnp.float32, jnp.bfloat16

    live = (jnp.arange(SEG, dtype=jnp.int32)[None, :] < lengths[:, None]).reshape(-1)
    live_f = live.astype(f32)
    flat_ids = expert_ids.reshape(-1)
    flat_live = jnp.repeat(live, routes)
    choice = flat_ids[:, None] == jnp.arange(z, dtype=jnp.int32)[None, :]
    onehot = (choice & flat_live[:, None]).astype(bf)
    order = jnp.arange(tokens * routes, dtype=jnp.int32)
    earlier = (order[None, :] < order[:, None]).astype(bf)
    before = jnp.dot(earlier, onehot, preferred_element_type=f32)
    pos = jnp.sum(before * choice.astype(f32), axis=1).astype(jnp.int32)
    counts = jnp.sum(onehot.astype(f32), axis=0)
    counts_tile = jnp.pad(counts[None, :], ((0, 7), (0, 128 - z)))
    stacked, gates, stats_tile, all_counts = router_terms(
        n,
        z,
        (policy_hidden, reference_hidden),
        (policy_norm_gain[None, :], reference_norm_gain[None, :]),
        (policy_router.T, reference_router.T),
        expert_ids.T,
        live_f[None, :],
        counts_tile,
    )
    block_counts = all_counts[:, 0, :z].astype(jnp.int32)
    totals = jnp.sum(block_counts, axis=0)
    mine = lax.dynamic_slice_in_dim(block_counts, ex, 1, axis=1)[:, 0]
    first = jnp.cumsum(mine) - mine
    weights = (
        (policy_gate[0], policy_up[0], policy_down[0]),
        (reference_gate[0], reference_up[0], reference_down[0]),
    )

    def layer(held, chunk, collective, single):
        target = jnp.where(flat_live, flat_ids * held + pos, -1).reshape(tokens, routes)
        slot = jnp.arange(z * held, dtype=jnp.int32)
        select = sum(slot[:, None] == target[:, k][None, :] for k in range(routes)).astype(bf)
        placed = jnp.dot(select, stacked, preferred_element_type=f32).astype(bf)
        within = jnp.arange(held, dtype=jnp.int32)
        packed = jnp.where(
            within[None, :] < mine[:, None], first[:, None] + within[None, :], -1
        ).reshape(-1)

        picks = jnp.stack(
            [(target[:, k][:, None] == slot[None, :]).astype(bf) for k in range(routes)]
        )

        def one_chunk(index):
            wanted = index * chunk + jnp.arange(chunk, dtype=jnp.int32)
            gather = (wanted[:, None] == packed[None, :]).astype(bf)
            spread = (packed[:, None] == wanted[None, :]).astype(bf)
            return experts(
                n, z, held, chunk, collective, placed, gather, spread, stats_tile, picks, gates, weights
            )

        def body(index, carry):
            mixed, all_stats = one_chunk(index)
            return carry[0] + mixed, all_stats

        if single:
            return one_chunk(0)
        zeros = (
            jnp.zeros((2, tokens, features), f32),
            jnp.zeros((n,) + stats_tile.shape, f32),
        )
        return lax.fori_loop(0, (need + chunk - 1) // chunk, body, zeros)

    need, need_held = jnp.max(totals), jnp.max(block_counts)
    sizes = []
    for part, rows in SIZES:
        size = (-(-part * cap // 6 // 16) * 16, -(-rows * n * cap // 48 // 16) * 16)
        if size not in sizes:
            sizes.append(size)
    branch = sum(
        ((need > chunk) | (need_held > held)).astype(jnp.int32) for held, chunk in sizes
    )
    branches = [
        functools.partial(layer, held, chunk, 1 + index, True)
        for index, (held, chunk) in enumerate(sizes)
    ] + [functools.partial(layer, *sizes[-1], len(sizes), False)]
    mixed, all_stats = lax.switch(branch, branches)
    stats = jnp.sum(all_stats, axis=(0, 2))
    balance = z * jnp.sum(
        totals.astype(f32) / (routes * token_total) * stats[:z] / token_total
    )
    lead = stats_tile.shape[0] - 8
    loss = KL_WEIGHT * stats[lead] / token_total + BALANCE_WEIGHT * balance
    return (mixed[0].astype(bf), mixed[1].astype(bf), stats_tile[lead], loss)


def solution(mesh):
    in_specs = (
        P("dp", "expert"),
        P("dp", "expert"),
        P("expert"),
        P("expert"),
        P("expert", None),
        P("expert", None),
        P("expert", "dp", None),
        P("expert", "dp", None),
        P("expert", "dp", None),
        P("expert", "dp", None),
        P("expert", "dp", None),
        P("expert", "dp", None),
        P("dp", None),
        P("dp"),
    )
    out_specs = (P("dp", "expert"), P("dp", "expert"), P("dp"), P())
    return jax.shard_map(
        per_device, mesh=mesh, in_specs=in_specs, out_specs=out_specs, check_vma=False
    )
```
